32 devices in a mesh: tm: 4 (over y, x), row: 4 (over z), col: 2 (over core).
Axes of the slice: x: 2, y: 2, z: 4, core: 2. Of those that a mesh axis runs over, the one named last changes fastest.
Arguments:
- noisy_video: float32 [16, 512, 512], P('tm', 'row', 'col'), may hold values from -6 to 6
- fidelity: float32 [16, 512, 512], P('tm', 'row', 'col'), may hold values from 0.5 to 12, as said below
Outputs:
- denoised: float32 [16, 512, 512], P('tm', 'row', 'col')
- gaps: float32 [3], replicated
The draws below stay inside these ranges and needn't reach their ends.
Inputs may be any that keep to these rules, and one draw needn't show every extreme that they name: `fidelity`: positive, larger on average toward later rows.
All inputs are finite; a program needn't handle non-finite values.
Results may differ from the reference program's by a relative error of at most 0.0001.
Values sent between devices are 32-bit elements; how exact they have to be, the bound alone decides.
A program may use at most 64 MiB of HBM per device.

```python
import math
import jax
import jax.numpy as jnp
from jax import lax

ITERS = 3
NT = 16
NH = 512
NW = 512


def draw_fidelity(key, part):
    inner = jax.random.fold_in(key, 11)
    base = jnp.exp(jax.random.uniform(inner, (NT, NH, NW), jnp.float32, math.log(0.5), math.log(4.0)))
    ramp = jnp.power(3.0, jnp.arange(NH, dtype=jnp.float32) / float(NH))
    return (base * ramp[None, :, None]).astype(jnp.float32)


def shard_levels(stream_key, dims, split, smallest, top_value):
    def one(dim, shards_of):
        steps = jax.random.uniform(jax.random.fold_in(jax.random.fold_in(stream_key, 6), dim), (shards_of,), jnp.float32, smallest / len(split), top_value / len(split))
        return jnp.repeat(jnp.exp(steps), dims[dim] // shards_of).reshape((-1,) + (1,) * (len(dims) - dim - 1))

    loudness = one(*split[0])
    for cut in split[1:]:
        loudness = loudness * one(*cut)
    return loudness


def normal_values(rng, dims, width, bound, cuts=(), kind=jnp.bfloat16):
    factor_of = shard_levels(rng, dims, cuts, -0.22, 0.18) if cuts else 1.0
    drawn = jax.random.normal(rng, dims, jnp.float32) * width * factor_of
    return jnp.minimum(jnp.maximum(drawn, -bound), bound).astype(kind)


def setup_inputs(seed: int = 0) -> dict:
    splits = jax.random.split(jax.random.key(seed), 3)
    noisy_video = normal_values(splits[0], (NT, NH, NW), 1.0, 6.0, ((0, 4), (1, 4), (2, 2)), jnp.float32)
    fidelity = draw_fidelity(jax.random.fold_in(splits[2], 71), 0)
    return dict(noisy_video=noisy_video, fidelity=fidelity)


sigma_step = 0.28
tau_step = 0.28

def forward(field, axis):
    count = field.shape[axis]
    ahead = lax.slice_in_dim(field, 1, count, axis=axis) - lax.slice_in_dim(field, 0, count - 1, axis=axis)
    edge = jnp.zeros_like(lax.slice_in_dim(field, 0, 1, axis=axis))
    return jnp.concatenate([ahead, edge], axis=axis)

def backward(comp, axis):
    count = comp.shape[axis]
    edge = jnp.zeros_like(lax.slice_in_dim(comp, 0, 1, axis=axis))
    before = jnp.concatenate([edge, lax.slice_in_dim(comp, 0, count - 1, axis=axis)], axis=axis)
    return comp - before

def reference(noisy_video, fidelity):
    field = noisy_video
    ubar_field = noisy_video
    zero_field = jnp.zeros_like(noisy_video)
    duals = [zero_field, zero_field, zero_field]
    grad_u = None
    gap_list = []
    for iteration in range(ITERS):
        grads = [forward(ubar_field, 0), forward(ubar_field, 1), forward(ubar_field, 2)]
        if iteration == 0:
            grad_u = grads
        else:
            grad_u = [0.5 * (grads[0] + grad_u[0]), 0.5 * (grads[1] + grad_u[1]), 0.5 * (grads[2] + grad_u[2])]
        moved = [duals[0] + sigma_step * grads[0], duals[1] + sigma_step * grads[1], duals[2] + sigma_step * grads[2]]
        length = jnp.sqrt(moved[0] * moved[0] + moved[1] * moved[1] + moved[2] * moved[2])
        scale = jnp.maximum(1.0, length)
        duals = [moved[0] / scale, moved[1] / scale, moved[2] / scale]
        diverge = backward(duals[0], 0) + backward(duals[1], 1) + backward(duals[2], 2)
        total_var = jnp.sqrt(grad_u[0] * grad_u[0] + grad_u[1] * grad_u[1] + grad_u[2] * grad_u[2])
        resid = field - noisy_video
        term = 0.5 * fidelity * resid * resid + total_var + diverge * diverge / (2.0 * fidelity) + noisy_video * diverge
        gap_list.append(jnp.sum(term) / float(term.size))
        new_field = (field + tau_step * diverge + tau_step * fidelity * noisy_video) / (1.0 + tau_step * fidelity)
        ubar_field = 2.0 * new_field - field
        field = new_field
    return (field, jnp.stack(gap_list).astype(jnp.float32))
```

```python
import functools

import jax
import jax.numpy as jnp
from jax import lax
from jax.experimental import pallas as pl
from jax.experimental.pallas import tpu as pltpu
from jax.sharding import PartitionSpec as P

ITERS = 3
SIGMA = 0.28
TAU = 0.28
MESH = pl.DeviceIdType.MESH

ROW_TO = ((0, -1, 0), (0, 1, 0), (1, -1, 0), (-1, 1, 0))
COL_TO = ((0, 0, -1), (0, 0, 1), (1, 0, -1), (-1, 0, 1), (0, 1, -1), (0, -1, 1))
FRAME_TO = ((-1, 0, 0), (1, 0, 0))


def kernel(
    sizes, groups, f_hbm, lam_hbm, out_hbm, gaps_ref,
    ub, lam, inv_lam, inv_den, uus, p0s, p1s, p2s, gus, es,
    pr, pc, hc, mp, sr, sc, rsr, rsc, gsend, grecv,
    ld_sem, out_sem, fs_sem, fr_sem, rs_sem, rr_sem, cs_sem, cr_sem, gs_sem, gr_sem,
):
    nt, nr, nc = sizes
    n = nt * nr * nc
    frames, rows, cols = f_hbm.shape
    it, ir, ic = lax.axis_index("tm"), lax.axis_index("row"), lax.axis_index("col")
    me = (it * nr + ir) * nc + ic
    per = rows // groups
    chunks = per // 8
    half = cols // 128
    f32 = jnp.float32

    def exists(off):
        cond = None
        for pos, size, d in zip((it, ir, ic), sizes, off):
            if d:
                c = pos + d < size if d > 0 else pos > 0
                cond = c if cond is None else jnp.logical_and(cond, c)
        return cond

    def place(off):
        return tuple(
            jnp.clip(pos + d, 0, size - 1) if d else pos
            for pos, size, d in zip((it, ir, ic), sizes, off)
        )

    def device(index):
        return (index // (nr * nc), (index // nc) % nr, index % nc)

    load_f = [
        pltpu.make_async_copy(
            f_hbm.at[t], ub[0].at[t + 1, pl.ds(0, rows), pl.ds(0, cols)], ld_sem.at[t]
        )
        for t in range(frames)
    ]
    load_lam = pltpu.make_async_copy(lam_hbm, lam, ld_sem.at[frames])
    for t in (0, frames - 1, *range(1, frames - 1)):
        load_f[t].start()
    load_lam.start()

    barrier = pltpu.get_barrier_semaphore()

    def greet(j, carry):
        pl.semaphore_signal(
            barrier, inc=1, device_id=device((me + j) % n), device_id_type=MESH
        )
        return carry

    lax.fori_loop(1, n, greet, 0)

    def row_copy(k, i):
        return pltpu.make_async_remote_copy(
            sr.at[k], rsr.at[k, i], rs_sem.at[k, i], rr_sem.at[k, i],
            device_id=place(ROW_TO[i]), device_id_type=MESH,
        )

    def col_copy(k, i):
        return pltpu.make_async_remote_copy(
            sc.at[k], rsc.at[k, i], cs_sem.at[k, i], cr_sem.at[k, i],
            device_id=place(COL_TO[i]), device_id_type=MESH,
        )

    def frame_copy(k, i, g):
        src_frame, dst_frame = ((1, frames + 1), (frames, 0))[i]
        part = pl.ds(pl.multiple_of(g * per, 8), per)
        return pltpu.make_async_remote_copy(
            ub[k].at[src_frame, part, pl.ds(0, cols)],
            ub[k].at[dst_frame, part, pl.ds(0, cols)],
            fs_sem.at[k, i, g], fr_sem.at[k, i, g],
            device_id=place(FRAME_TO[i]), device_id_type=MESH,
        )

    def back(off):
        return tuple(-d for d in off)

    def send_frames(k, g):
        for i in (0, 1):
            @pl.when(exists(FRAME_TO[i]))
            def _(i=i):
                frame_copy(k, i, g).start()

    def wait_frames(k, g):
        for i in (0, 1):
            @pl.when(exists(back(FRAME_TO[i])))
            def _(i=i):
                frame_copy(k, i, g).wait_recv()

    def send_small(k):
        for t in range(frames):
            sr[k, t : t + 1, :] = ub[k][t + 1, 0:1, 0:cols]
            sr[k, frames + t : frames + t + 1, :] = ub[k][t + 1, rows - 1 : rows, 0:cols]
        for i in range(len(ROW_TO)):
            @pl.when(exists(ROW_TO[i]))
            def _(i=i):
                row_copy(k, i).start()
        sc[k] = mp[...].T[0:8, :]
        for i in range(len(COL_TO)):
            @pl.when(exists(COL_TO[i]))
            def _(i=i):
                col_copy(k, i).start()

    def wait_small(k):
        for i in range(len(ROW_TO)):
            @pl.when(exists(back(ROW_TO[i])))
            def _(i=i):
                row_copy(k, i).wait_recv()
        for i in range(len(COL_TO)):
            @pl.when(exists(back(COL_TO[i])))
            def _(i=i):
                col_copy(k, i).wait_recv()

    lane = lax.broadcasted_iota(jnp.int32, (8, 128), 1)
    sub = lax.broadcasted_iota(jnp.int32, (8, 128), 0)
    lane_w = lax.broadcasted_iota(jnp.int32, (8, cols), 1)
    sub_w = lax.broadcasted_iota(jnp.int32, (8, cols), 0)
    end_t, end_r, end_c = it == nt - 1, ir == nr - 1, ic == nc - 1

    def pack_cols(firsts, lasts):
        packed = jnp.zeros((8, 128), f32)
        for t in range(frames):
            packed = jnp.where(lane == t, pltpu.roll(firsts[t], t, 1) if t else firsts[t], packed)
            packed = jnp.where(lane == frames + t, pltpu.roll(lasts[t], frames + t + 1, 1), packed)
        return packed

    for c in load_f:
        c.wait()

    def first_pack(c, carry):
        r = pl.ds(pl.multiple_of(c * 8, 8), 8)
        mp[r, :] = pack_cols(
            [ub[0][t + 1, r, 0:128] for t in range(frames)],
            [ub[0][t + 1, r, cols - 128 : cols] for t in range(frames)],
        )
        return carry

    lax.fori_loop(0, rows // 8, first_pack, 0)
    pl.semaphore_wait(barrier, n - 1)
    send_small(0)
    for g in range(groups):
        send_frames(0, g)
    load_lam.wait()

    def prepare(c, carry):
        r = pl.ds(pl.multiple_of(c * 8, 8), 8)
        for t in range(frames):
            value = lam[t, r, :]
            inv_lam[t, r, :] = 0.5 / value
            inv_den[t, r, :] = 1.0 / (1.0 + TAU * value)
        return carry

    lax.fori_loop(0, rows // 8, prepare, 0)

    def shrink(m):
        s = jnp.minimum(1.0, lax.rsqrt(m[0] * m[0] + m[1] * m[1] + m[2] * m[2]))
        return [v * s for v in m]

    def edge_duals(k):
        a = rsr[k, 1]
        ahead_t = jnp.where(sub_w == 7, pltpu.roll(rsr[k, 3], 3, 0), pltpu.roll(a, 7, 0))
        corner = pltpu.roll(rsc[k, 4], 4, 0)[:, 127:128]
        ahead_c = jnp.where(lane_w == cols - 1, corner, pltpu.roll(a, cols - 1, 1))
        g = [
            jnp.where(jnp.logical_and(sub_w == 7, end_t), 0.0, ahead_t - a),
            pltpu.roll(sr[k], 4, 0) - a,
            jnp.where(jnp.logical_and(lane_w == cols - 1, end_c), 0.0, ahead_c - a),
        ]
        m = [SIGMA * v if k == 0 else pr[d] + SIGMA * v for d, v in enumerate(g)]
        m = shrink(m)
        for d in range(3):
            pr[d] = m[d]
        above = jnp.where(ir > 0, m[1], 0.0)
        for t in range(frames):
            p1s[k][t + 1][7:8, :] = above[frames + t : frames + t + 1, :]
        b = rsc[k, 1]
        ahead_t = jnp.where(sub == 7, pltpu.roll(rsc[k, 3], 3, 0), pltpu.roll(b, 7, 0))
        corner = rsc[k, 5][:, 0:1]
        ahead_r = jnp.where(lane == 127, corner, pltpu.roll(b, 127, 1))
        g = [
            jnp.where(jnp.logical_and(sub == 7, end_t), 0.0, ahead_t - b),
            jnp.where(jnp.logical_and(lane == 127, end_r), 0.0, ahead_r - b),
            pltpu.roll(sc[k], 4, 0) - b,
        ]
        m = [SIGMA * v if k == 0 else pc[d] + SIGMA * v for d, v in enumerate(g)]
        m = shrink(m)
        for d in range(3):
            pc[d] = m[d]
        left = jnp.where(ic > 0, m[2], 0.0)
        right = jnp.where(sub == frames, pltpu.roll(rsc[k, 2], 1, 0), rsc[k, 0])
        hc[...] = jnp.concatenate(
            [right, left, jnp.zeros((112, 128), f32)], axis=0
        ).T
        for t in range(frames):
            ub[k][t + 1, rows : rows + 1, 0:cols] = rsr[k, 0, t : t + 1, :]
        ub[k][0, rows : rows + 1, 0:cols] = rsr[k, 2, frames - 1 : frames, :]

    def lanes(h):
        return pl.ds(h * 128, 128)

    def gap_term(g, e, noisy, inv, weight, u):
        term = jnp.sqrt(g[0] * g[0] + g[1] * g[1] + g[2] * g[2]) + e * (e * inv + noisy)
        if u is None:
            return term
        resid = u - noisy
        return term + 0.5 * weight * resid * resid

    def chunk(k, c, acc):
        r0 = pl.multiple_of(c * 8, 8)
        r = pl.ds(r0, 8)
        below = pl.ds(pl.multiple_of(r0 + 8, 8), 8)
        last_chunk_row = jnp.logical_and(jnp.logical_and(sub == 7, end_r), c == rows // 8 - 1)
        last_lane = jnp.logical_and(lane == 127, end_c)
        halo = hc[r, :]
        prev0 = None
        firsts, lasts = [], []
        x = [ub[k][0, r, lanes(h)] for h in range(half)]
        for j in range(frames + 1):
            t = j - 1
            xn = [ub[k][j + 1, r, lanes(h)] for h in range(half)]
            where_right = t if t >= 0 else frames
            right = jnp.broadcast_to(halo[:, where_right : where_right + 1], (8, 128))
            cur0, cur2 = [], []
            if t >= 0:
                prev1 = [p1s[k][j][r, lanes(h)] for h in range(half)]
            for h in range(half):
                g0 = xn[h] - x[h]
                if t == frames - 1:
                    g0 = jnp.where(end_t, 0.0, g0)
                g1 = pltpu.roll(jnp.where(sub == 0, ub[k][j, below, lanes(h)], x[h]), 7, 0) - x[h]
                g1 = jnp.where(last_chunk_row, 0.0, g1)
                follow = x[h + 1] if h + 1 < half else right
                g2 = pltpu.roll(jnp.where(lane == 0, follow, x[h]), 127, 1) - x[h]
                if h == half - 1:
                    g2 = jnp.where(last_lane, 0.0, g2)
                g = [g0, g1, g2]
                if k == 0:
                    m = [SIGMA * v for v in g]
                else:
                    m = [
                        p0s[k - 1][j, r, lanes(h)],
                        p1s[k - 1][j][below, lanes(h)],
                        p2s[k - 1][j, r, lanes(h)],
                    ]
                    m = [q + SIGMA * v for q, v in zip(m, g)]
                m = shrink(m)
                if k < ITERS - 1:
                    p0s[k][j, r, lanes(h)] = m[0]
                    p2s[k][j, r, lanes(h)] = m[2]
                p1s[k][j][below, lanes(h)] = m[1]
                cur0.append(m[0])
                cur2.append(m[2])
                if t < 0:
                    continue
                d0 = m[0] - prev0[h]
                d1 = m[1] - pltpu.roll(jnp.where(sub == 7, prev1[h], m[1]), 1, 0)
                if h == 0:
                    before = jnp.broadcast_to(halo[:, 8 + frames + t : 9 + frames + t], (8, 128))
                else:
                    before = cur2[h - 1]
                d2 = m[2] - pltpu.roll(jnp.where(lane == 127, before, m[2]), 1, 1)
                e = d0 + d1 + d2
                if k > 0:
                    g = [0.5 * (v + gus[k - 1][d][t, r, lanes(h)]) for d, v in enumerate(g)]
                if k < ITERS - 1:
                    for d in range(3):
                        gus[k][d][t, r, lanes(h)] = g[d]
                noisy = ub[0][j, r, lanes(h)]
                weight = lam[t, r, lanes(h)]
                u = noisy if k == 0 else uus[k - 1][t, r, lanes(h)]
                if k < ITERS - 1:
                    es[t, r, lanes(h)] = e
                else:
                    acc = acc + gap_term(g, e, noisy, inv_lam[t, r, lanes(h)], weight, u)
                new = (u + TAU * e + TAU * weight * noisy) * inv_den[t, r, lanes(h)]
                (out_hbm if k == ITERS - 1 else uus[k])[t, r, lanes(h)] = new
                if k < ITERS - 1:
                    ubar = 2.0 * new - u
                    ub[k + 1][j, r, lanes(h)] = ubar
                    if h == 0:
                        firsts.append(ubar)
                    if h == half - 1:
                        lasts.append(ubar)
            if t < 0:
                prev0 = [jnp.where(it > 0, v, 0.0) for v in cur0]
            else:
                prev0 = cur0
            x = xn
        if k < ITERS - 1:
            mp[r, :] = pack_cols(firsts, lasts)
        return acc

    def out_copy(g):
        part = pl.ds(pl.multiple_of(g * per, 8), per)
        return pltpu.make_async_copy(
            uus[ITERS - 1].at[:, part, :], out_hbm.at[:, part, :], out_sem.at[g]
        )

    def gap_chunk(k, c, acc):
        r = pl.ds(pl.multiple_of(c * 8, 8), 8)
        for t in range(frames):
            for h in range(half):
                at = (t, r, lanes(h))
                noisy = ub[0][t + 1, r, lanes(h)]
                acc = acc + gap_term(
                    [gus[k][d][at] for d in range(3)], es[at], noisy, inv_lam[at],
                    lam[at] if k else None, uus[k - 1][at] if k else None,
                )
        return acc

    local = jnp.zeros((1, 128), f32)
    lane_row = lax.broadcasted_iota(jnp.int32, (1, 128), 1)
    for k in range(ITERS):
        wait_small(k)
        edge_duals(k)
        wait_frames(k, 0)

        def group(g, acc, k=k):
            @pl.when(g + 1 < groups)
            def _():
                wait_frames(k, g + 1)

            acc = lax.fori_loop(
                0, chunks, lambda c, a: chunk(k, g * chunks + c, a), acc, unroll=4
            )
            if k < ITERS - 1:
                @pl.when(g < 1)
                def _():
                    send_frames(k + 1, g)
            else:
                pass
            return acc

        acc = lax.fori_loop(0, groups, group, jnp.zeros((8, 128), f32))
        if k < ITERS - 1:
            send_small(k + 1)
            for g in range(1, groups):
                send_frames(k + 1, g)
            acc = lax.fori_loop(
                0, rows // 8, functools.partial(gap_chunk, k), acc, unroll=2
            )
        total = jnp.sum(jnp.sum(acc, axis=0, keepdims=True), axis=1, keepdims=True)
        local = jnp.where(lane_row == k, total, local)

    gsend[0] = local

    def gap_copy(j):
        return pltpu.make_async_remote_copy(
            gsend.at[0], grecv.at[j - 1], gs_sem, gr_sem,
            device_id=device((me + j) % n), device_id_type=MESH,
        )

    def tell(j, carry):
        gap_copy(j).start()
        return carry

    lax.fori_loop(1, n, tell, 0)

    for k in range(ITERS):
        for i in range(len(ROW_TO)):
            @pl.when(exists(ROW_TO[i]))
            def _(k=k, i=i):
                row_copy(k, i).wait_send()
        for i in range(len(COL_TO)):
            @pl.when(exists(COL_TO[i]))
            def _(k=k, i=i):
                col_copy(k, i).wait_send()
        for i in (0, 1):
            @pl.when(exists(FRAME_TO[i]))
            def _(k=k, i=i):
                for g in range(groups):
                    frame_copy(k, i, g).wait_send()
    everything = grecv.at[pl.ds(0, n - 1)]
    pltpu.make_async_copy(everything, everything, gr_sem).wait()
    pltpu.make_async_copy(everything, everything, gs_sem).wait()

    total = local + jnp.sum(grecv[...], axis=0)
    total = total * (1.0 / float(n * frames * rows * cols))
    gaps_ref[...] = total[0, 0:ITERS]


def put(u, gaps, u_out, gaps_out, sem):
    copies = [
        pltpu.make_async_copy(u, u_out, sem.at[0]),
        pltpu.make_async_copy(gaps, gaps_out, sem.at[1]),
    ]
    for c in copies:
        c.start()
    for c in copies:
        c.wait()


def solution(mesh):
    sizes = (mesh.shape["tm"], mesh.shape["row"], mesh.shape["col"])
    n = sizes[0] * sizes[1] * sizes[2]

    def on_device(noisy_video, fidelity):
        frames, rows, cols = noisy_video.shape
        groups = 4
        block = (frames, rows, cols)
        dma = pltpu.SemaphoreType.DMA
        vm = lambda *shape: pltpu.VMEM(shape, jnp.float32)
        outs = pl.pallas_call(
            functools.partial(kernel, sizes, groups),
            out_shape=(
                pltpu.VMEM(block, jnp.float32),
                pltpu.VMEM((ITERS,), jnp.float32),
            ),
            in_specs=[pl.BlockSpec(memory_space=pltpu.HBM)] * 2,
            out_specs=(
                pl.BlockSpec(memory_space=pltpu.VMEM),
                pl.BlockSpec(memory_space=pltpu.VMEM),
            ),
            scratch_shapes=[
                [vm(frames + 2, rows + 8, cols) for _ in range(ITERS)],
                vm(*block), vm(*block), vm(*block),
                [vm(*block) for _ in range(ITERS)],
                [vm(frames + 1, rows, cols) for _ in range(ITERS - 1)],
                [[vm(rows + 8, cols) for _ in range(frames + 1)] for _ in range(ITERS)],
                [vm(frames + 1, rows, cols) for _ in range(ITERS - 1)],
                [[vm(*block) for _ in range(3)] for _ in range(ITERS - 1)],
                vm(*block),
                vm(3, 8, cols), vm(3, 8, 128), vm(rows, 128), vm(rows, 128),
                vm(ITERS, 8, cols), vm(ITERS, 8, 128),
                vm(ITERS, len(ROW_TO), 8, cols), vm(ITERS, len(COL_TO), 8, 128),
                vm(1, 1, 128), vm(n - 1, 1, 128),
                dma((frames + 1,)), dma((groups,)),
                dma((ITERS, 2, groups)), dma((ITERS, 2, groups)),
                dma((ITERS, len(ROW_TO))), dma((ITERS, len(ROW_TO))),
                dma((ITERS, len(COL_TO))), dma((ITERS, len(COL_TO))),
                dma(()), dma(()),
            ],
            compiler_params=pltpu.CompilerParams(
                collective_id=0, has_side_effects=True
            ),
            name="chambolle_pock",
        )(noisy_video, fidelity)
        return pl.pallas_call(
            put,
            out_shape=(
                jax.ShapeDtypeStruct(block, jnp.float32),
                jax.ShapeDtypeStruct((ITERS,), jnp.float32),
            ),
            in_specs=[pl.BlockSpec(memory_space=pltpu.VMEM)] * 2,
            out_specs=[pl.BlockSpec(memory_space=pltpu.HBM)] * 2,
            scratch_shapes=[dma((2,))],
            name="put",
        )(*[pltpu.with_memory_space_constraint(x, pltpu.VMEM) for x in outs])

    return jax.shard_map(
        on_device,
        mesh=mesh,
        in_specs=(P("tm", "row", "col"), P("tm", "row", "col")),
        out_specs=(P("tm", "row", "col"), P()),
        check_vma=False,
    )
```

```python
import functools

import jax
import jax.numpy as jnp
from jax import lax
from jax.experimental import pallas as pl
from jax.experimental.pallas import tpu as pltpu
from jax.sharding import PartitionSpec as P

ITERS = 3
SIGMA = 0.28
TAU = 0.28
MESH = pl.DeviceIdType.MESH

ROW_TO = ((0, -1, 0), (0, 1, 0), (1, -1, 0), (-1, 1, 0))
COL_TO = ((0, 0, -1), (0, 0, 1), (1, 0, -1), (-1, 0, 1), (0, 1, -1), (0, -1, 1))
FRAME_TO = ((-1, 0, 0), (1, 0, 0))


def kernel(
    sizes, groups, f_hbm, lam_hbm, out_hbm, gaps_ref,
    ub, lam, inv_lam, inv_den, uus, p0s, p1s, p2s, gus, es,
    pr, pc, hc, mp, sr, sc, rsr, rsc, gsend, grecv,
    ld_sem, fs_sem, fr_sem, rs_sem, rr_sem, cs_sem, cr_sem, gs_sem, gr_sem, hello_sem,
):
    nt, nr, nc = sizes
    n = nt * nr * nc
    frames, rows, cols = f_hbm.shape
    it, ir, ic = lax.axis_index("tm"), lax.axis_index("row"), lax.axis_index("col")
    me = (it * nr + ir) * nc + ic
    per = rows // groups
    chunks = per // 8
    half = cols // 128
    f32 = jnp.float32

    def exists(off):
        cond = None
        for pos, size, d in zip((it, ir, ic), sizes, off):
            if d:
                c = pos + d < size if d > 0 else pos > 0
                cond = c if cond is None else jnp.logical_and(cond, c)
        return cond

    def place(off):
        return tuple(
            jnp.clip(pos + d, 0, size - 1) if d else pos
            for pos, size, d in zip((it, ir, ic), sizes, off)
        )

    def device(index):
        return (index // (nr * nc), (index // nc) % nr, index % nc)

    def back(off):
        return tuple(-d for d in off)

    def how_many(offsets):
        return sum(jnp.where(exists(off), 1, 0) for off in offsets)

    def wait_for(count, most, sem, region):
        for c in range(1, most + 1):
            @pl.when(count == c)
            def _(c=c):
                pltpu.make_async_copy(region(c), region(c), sem).wait()

    row_out, row_in = how_many(ROW_TO), how_many([back(o) for o in ROW_TO])
    col_out, col_in = how_many(COL_TO), how_many([back(o) for o in COL_TO])
    frame_out = how_many(FRAME_TO)

    barrier = pltpu.get_barrier_semaphore()
    near = ROW_TO + COL_TO + FRAME_TO
    for off in near:
        @pl.when(exists(off))
        def _(off=off):
            pl.semaphore_signal(
                barrier, inc=1, device_id=place(off), device_id_type=MESH
            )

    load_f = [
        pltpu.make_async_copy(
            f_hbm.at[t], ub[0].at[t + 1, pl.ds(0, rows), pl.ds(0, cols)], ld_sem.at[0]
        )
        for t in range(frames)
    ]
    load_lam = pltpu.make_async_copy(lam_hbm, lam, ld_sem.at[1])
    for t in range(frames):
        load_f[t].start()
    load_lam.start()

    rounds = [1] * (nr - 2) + [2] * (nc - 1) + [0] * (nt - 1)

    def hello_to(r):
        axis = rounds[r]
        return [tuple(d if a == axis else 0 for a in range(3)) for d in (-1, 1)]

    def say_hello(r):
        if r < len(rounds):
            for off in hello_to(r):
                @pl.when(exists(off))
                def _(off=off):
                    pl.semaphore_signal(
                        hello_sem.at[r], inc=1, device_id=place(off), device_id_type=MESH
                    )

    def hear_hello(r):
        if 0 <= r < len(rounds):
            pl.semaphore_wait(hello_sem.at[r], how_many(hello_to(r)))

    def next_hello(r):
        hear_hello(r - 1)
        say_hello(r)

    def row_copy(k, i):
        return pltpu.make_async_remote_copy(
            sr.at[k], rsr.at[k, i], rs_sem.at[0], rr_sem.at[k],
            device_id=place(ROW_TO[i]), device_id_type=MESH,
        )

    def col_copy(k, i):
        return pltpu.make_async_remote_copy(
            sc.at[k], rsc.at[k, i], cs_sem.at[0], cr_sem.at[k],
            device_id=place(COL_TO[i]), device_id_type=MESH,
        )

    def frame_copy(k, i, g):
        src_frame, dst_frame = ((1, frames + 1), (frames, 0))[i]
        part = pl.ds(pl.multiple_of(g * per, 8), per)
        return pltpu.make_async_remote_copy(
            ub[k].at[src_frame, part, pl.ds(0, cols)],
            ub[k].at[dst_frame, part, pl.ds(0, cols)],
            fs_sem.at[k], fr_sem.at[k, g],
            device_id=place(FRAME_TO[i]), device_id_type=MESH,
        )

    def send_frames(k, g):
        for i in (0, 1):
            @pl.when(exists(FRAME_TO[i]))
            def _(i=i):
                frame_copy(k, i, g).start()

    def wait_frames(k, g):
        part = pl.ds(pl.multiple_of(g * per, 8), per)
        wait_for(
            frame_out, 2, fr_sem.at[k, g],
            lambda c: ub[k].at[pl.ds(0, c), part, pl.ds(0, cols)],
        )

    def send_rows(k):
        for t in range(frames):
            sr[k, t : t + 1, :] = ub[k][t + 1, 0:1, 0:cols]
            sr[k, frames + t : frames + t + 1, :] = ub[k][t + 1, rows - 1 : rows, 0:cols]
        for i in range(len(ROW_TO)):
            @pl.when(exists(ROW_TO[i]))
            def _(i=i):
                row_copy(k, i).start()

    def send_cols(k):
        sc[k] = mp[...].T[0:8, :]
        for i in range(len(COL_TO)):
            @pl.when(exists(COL_TO[i]))
            def _(i=i):
                col_copy(k, i).start()

    def send_small(k):
        send_rows(k)
        send_cols(k)

    def wait_small(k):
        wait_for(row_in, len(ROW_TO), rr_sem.at[k], lambda c: rsr.at[k, pl.ds(0, c)])
        wait_for(col_in, len(COL_TO), cr_sem.at[k], lambda c: rsc.at[k, pl.ds(0, c)])

    lane = lax.broadcasted_iota(jnp.int32, (8, 128), 1)
    sub = lax.broadcasted_iota(jnp.int32, (8, 128), 0)
    lane_w = lax.broadcasted_iota(jnp.int32, (8, cols), 1)
    sub_w = lax.broadcasted_iota(jnp.int32, (8, cols), 0)
    end_t, end_r, end_c = it == nt - 1, ir == nr - 1, ic == nc - 1

    def pack_cols(firsts, lasts):
        packed = jnp.zeros((8, 128), f32)
        for t in range(frames):
            packed = jnp.where(lane == t, pltpu.roll(firsts[t], t, 1) if t else firsts[t], packed)
            packed = jnp.where(lane == frames + t, pltpu.roll(lasts[t], frames + t + 1, 1), packed)
        return packed

    loaded = ub[0].at[pl.ds(1, frames), pl.ds(0, rows), pl.ds(0, cols)]
    pltpu.make_async_copy(loaded, loaded, ld_sem.at[0]).wait()

    def first_pack(c, carry):
        r = pl.ds(pl.multiple_of(c * 8, 8), 8)
        mp[r, :] = pack_cols(
            [ub[0][t + 1, r, 0:128] for t in range(frames)],
            [ub[0][t + 1, r, cols - 128 : cols] for t in range(frames)],
        )
        return carry

    lax.fori_loop(0, rows // 8, first_pack, 0, unroll=8)
    pl.semaphore_wait(barrier, how_many(near))
    send_small(0)
    for g in range(groups):
        send_frames(0, g)
    say_hello(0)
    load_lam.wait()

    def prepare(c, carry):
        r = pl.ds(pl.multiple_of(c * 8, 8), 8)
        for t in range(frames):
            value = lam[t, r, :]
            inv_lam[t, r, :] = 0.5 / value
            inv_den[t, r, :] = 1.0 / (1.0 + TAU * value)
        return carry

    lax.fori_loop(0, rows // 8, prepare, 0)

    def shrink(m):
        s = jnp.minimum(1.0, lax.rsqrt(m[0] * m[0] + m[1] * m[1] + m[2] * m[2]))
        return [v * s for v in m]

    def edge_duals(k):
        a = rsr[k, 1]
        ahead_t = jnp.where(sub_w == 7, pltpu.roll(rsr[k, 3], 3, 0), pltpu.roll(a, 7, 0))
        corner = pltpu.roll(rsc[k, 4], 4, 0)[:, 127:128]
        ahead_c = jnp.where(lane_w == cols - 1, corner, pltpu.roll(a, cols - 1, 1))
        g = [
            jnp.where(jnp.logical_and(sub_w == 7, end_t), 0.0, ahead_t - a),
            pltpu.roll(sr[k], 4, 0) - a,
            jnp.where(jnp.logical_and(lane_w == cols - 1, end_c), 0.0, ahead_c - a),
        ]
        m = [SIGMA * v if k == 0 else pr[d] + SIGMA * v for d, v in enumerate(g)]
        m = shrink(m)
        for d in range(3):
            pr[d] = m[d]
        above = jnp.where(ir > 0, m[1], 0.0)
        for t in range(frames):
            p1s[k][t + 1][7:8, :] = above[frames + t : frames + t + 1, :]
        b = rsc[k, 1]
        ahead_t = jnp.where(sub == 7, pltpu.roll(rsc[k, 3], 3, 0), pltpu.roll(b, 7, 0))
        corner = rsc[k, 5][:, 0:1]
        ahead_r = jnp.where(lane == 127, corner, pltpu.roll(b, 127, 1))
        g = [
            jnp.where(jnp.logical_and(sub == 7, end_t), 0.0, ahead_t - b),
            jnp.where(jnp.logical_and(lane == 127, end_r), 0.0, ahead_r - b),
            pltpu.roll(sc[k], 4, 0) - b,
        ]
        m = [SIGMA * v if k == 0 else pc[d] + SIGMA * v for d, v in enumerate(g)]
        m = shrink(m)
        for d in range(3):
            pc[d] = m[d]
        left = jnp.where(ic > 0, m[2], 0.0)
        right = jnp.where(sub == frames, pltpu.roll(rsc[k, 2], 1, 0), rsc[k, 0])
        hc[...] = jnp.concatenate(
            [right, left, jnp.zeros((112, 128), f32)], axis=0
        ).T
        for t in range(frames):
            ub[k][t + 1, rows : rows + 1, 0:cols] = rsr[k, 0, t : t + 1, :]
        ub[k][0, rows : rows + 1, 0:cols] = rsr[k, 2, frames - 1 : frames, :]

    def lanes(h):
        return pl.ds(h * 128, 128)

    def gap_term(g, e, noisy, inv, weight, u):
        term = jnp.sqrt(g[0] * g[0] + g[1] * g[1] + g[2] * g[2]) + e * (e * inv + noisy)
        if u is None:
            return term
        resid = u - noisy
        return term + 0.5 * weight * resid * resid

    def chunk(k, c, acc):
        r0 = pl.multiple_of(c * 8, 8)
        r = pl.ds(r0, 8)
        below = pl.ds(pl.multiple_of(r0 + 8, 8), 8)
        last_chunk_row = jnp.logical_and(jnp.logical_and(sub == 7, end_r), c == rows // 8 - 1)
        last_lane = jnp.logical_and(lane == 127, end_c)
        halo = hc[r, :]
        prev0 = None
        firsts, lasts = [], []
        x = [ub[k][0, r, lanes(h)] for h in range(half)]
        for j in range(frames + 1):
            t = j - 1
            xn = [ub[k][j + 1, r, lanes(h)] for h in range(half)]
            where_right = t if t >= 0 else frames
            right = jnp.broadcast_to(halo[:, where_right : where_right + 1], (8, 128))
            cur0, cur2 = [], []
            if t >= 0:
                prev1 = [p1s[k][j][r, lanes(h)] for h in range(half)]
            for h in range(half):
                g0 = xn[h] - x[h]
                if t == frames - 1:
                    g0 = jnp.where(end_t, 0.0, g0)
                g1 = pltpu.roll(jnp.where(sub == 0, ub[k][j, below, lanes(h)], x[h]), 7, 0) - x[h]
                g1 = jnp.where(last_chunk_row, 0.0, g1)
                follow = x[h + 1] if h + 1 < half else right
                g2 = pltpu.roll(jnp.where(lane == 0, follow, x[h]), 127, 1) - x[h]
                if h == half - 1:
                    g2 = jnp.where(last_lane, 0.0, g2)
                g = [g0, g1, g2]
                if k == 0:
                    m = [SIGMA * v for v in g]
                else:
                    m = [
                        p0s[k - 1][j, r, lanes(h)],
                        p1s[k - 1][j][below, lanes(h)],
                        p2s[k - 1][j, r, lanes(h)],
                    ]
                    m = [q + SIGMA * v for q, v in zip(m, g)]
                m = shrink(m)
                if k < ITERS - 1:
                    p0s[k][j, r, lanes(h)] = m[0]
                    p2s[k][j, r, lanes(h)] = m[2]
                p1s[k][j][below, lanes(h)] = m[1]
                cur0.append(m[0])
                cur2.append(m[2])
                if t < 0:
                    continue
                d0 = m[0] - prev0[h]
                d1 = m[1] - pltpu.roll(jnp.where(sub == 7, prev1[h], m[1]), 1, 0)
                if h == 0:
                    before = jnp.broadcast_to(halo[:, 8 + frames + t : 9 + frames + t], (8, 128))
                else:
                    before = cur2[h - 1]
                d2 = m[2] - pltpu.roll(jnp.where(lane == 127, before, m[2]), 1, 1)
                e = d0 + d1 + d2
                if k > 0:
                    g = [0.5 * (v + gus[k - 1][d][t, r, lanes(h)]) for d, v in enumerate(g)]
                if k < ITERS - 1:
                    for d in range(3):
                        gus[k][d][t, r, lanes(h)] = g[d]
                noisy = ub[0][j, r, lanes(h)]
                weight = lam[t, r, lanes(h)]
                u = noisy if k == 0 else uus[k - 1][t, r, lanes(h)]
                if k < ITERS - 1:
                    es[t, r, lanes(h)] = e
                else:
                    acc = acc + gap_term(g, e, noisy, inv_lam[t, r, lanes(h)], weight, u)
                new = (u + TAU * e + TAU * weight * noisy) * inv_den[t, r, lanes(h)]
                (out_hbm if k == ITERS - 1 else uus[k])[t, r, lanes(h)] = new
                if k < ITERS - 1:
                    ubar = 2.0 * new - u
                    ub[k + 1][j, r, lanes(h)] = ubar
                    if h == 0:
                        firsts.append(ubar)
                    if h == half - 1:
                        lasts.append(ubar)
            if t < 0:
                prev0 = [jnp.where(it > 0, v, 0.0) for v in cur0]
            else:
                prev0 = cur0
            x = xn
        if k < ITERS - 1:
            mp[r, :] = pack_cols(firsts, lasts)
        return acc

    def gap_chunk(k, c, acc):
        r = pl.ds(pl.multiple_of(c * 8, 8), 8)
        for t in range(frames):
            for h in range(half):
                at = (t, r, lanes(h))
                noisy = ub[0][t + 1, r, lanes(h)]
                acc = acc + gap_term(
                    [gus[k][d][at] for d in range(3)], es[at], noisy, inv_lam[at],
                    lam[at] if k else None, uus[k - 1][at] if k else None,
                )
        return acc

    local = jnp.zeros((1, 128), f32)
    lane_row = lax.broadcasted_iota(jnp.int32, (1, 128), 1)
    for k in range(ITERS):
        wait_small(k)
        edge_duals(k)
        next_hello(2 * k + 1)
        wait_frames(k, 0)

        def group(g, acc, k=k):
            @pl.when(g + 1 < groups)
            def _():
                wait_frames(k, g + 1)

            acc = lax.fori_loop(
                0, chunks, lambda c, a: chunk(k, g * chunks + c, a), acc, unroll=4
            )
            if k < ITERS - 1:
                @pl.when(g < 1)
                def _():
                    send_frames(k + 1, g)
            return acc

        acc = lax.fori_loop(0, groups, group, jnp.zeros((8, 128), f32))
        next_hello(2 * k + 2)
        if k < ITERS - 1:
            send_small(k + 1)
            for g in range(1, groups):
                send_frames(k + 1, g)
            acc = lax.fori_loop(
                0, rows // 8, functools.partial(gap_chunk, k), acc, unroll=2
            )
        total = jnp.sum(jnp.sum(acc, axis=0, keepdims=True), axis=1, keepdims=True)
        local = jnp.where(lane_row == k, total, local)

    for r in range(2 * ITERS, len(rounds)):
        next_hello(r + 1)

    gsend[0] = local

    def gap_copy(j):
        return pltpu.make_async_remote_copy(
            gsend.at[0], grecv.at[j - 1], gs_sem, gr_sem,
            device_id=device((me + j) % n), device_id_type=MESH,
        )

    def tell(b, carry):
        for c in range(spread):
            gap_copy(b * spread + c + 1).start()
        return carry

    spread = max(d for d in range(1, 33) if (n - 1) % d == 0)
    lax.fori_loop(0, (n - 1) // spread, tell, 0)

    wait_for(row_out, len(ROW_TO), rs_sem.at[0], lambda c: rsr.at[:, pl.ds(0, c)])
    wait_for(col_out, len(COL_TO), cs_sem.at[0], lambda c: rsc.at[:, pl.ds(0, c)])
    for k in range(ITERS):
        wait_for(
            frame_out, 2, fs_sem.at[k],
            lambda c, k=k: ub[k].at[pl.ds(0, c), pl.ds(0, rows), pl.ds(0, cols)],
        )
    everything = grecv.at[pl.ds(0, n - 1)]
    pltpu.make_async_copy(everything, everything, gr_sem).wait()
    pltpu.make_async_copy(everything, everything, gs_sem).wait()

    total = local + jnp.sum(grecv[...], axis=0)
    total = total * (1.0 / float(n * frames * rows * cols))
    gaps_ref[...] = total[0, 0:ITERS]


def put(u, gaps, u_out, gaps_out, sem):
    copies = [
        pltpu.make_async_copy(u, u_out, sem.at[0]),
        pltpu.make_async_copy(gaps, gaps_out, sem.at[1]),
    ]
    for c in copies:
        c.start()
    for c in copies:
        c.wait()


def solution(mesh):
    sizes = (mesh.shape["tm"], mesh.shape["row"], mesh.shape["col"])
    n = sizes[0] * sizes[1] * sizes[2]

    def on_device(noisy_video, fidelity):
        frames, rows, cols = noisy_video.shape
        groups = 4
        block = (frames, rows, cols)
        dma = pltpu.SemaphoreType.DMA
        vm = lambda *shape: pltpu.VMEM(shape, jnp.float32)
        outs = pl.pallas_call(
            functools.partial(kernel, sizes, groups),
            out_shape=(
                pltpu.VMEM(block, jnp.float32),
                pltpu.VMEM((ITERS,), jnp.float32),
            ),
            in_specs=[pl.BlockSpec(memory_space=pltpu.HBM)] * 2,
            out_specs=(
                pl.BlockSpec(memory_space=pltpu.VMEM),
                pl.BlockSpec(memory_space=pltpu.VMEM),
            ),
            scratch_shapes=[
                [vm(frames + 2, rows + 8, cols) for _ in range(ITERS)],
                vm(*block), vm(*block), vm(*block),
                [vm(*block) for _ in range(ITERS)],
                [vm(frames + 1, rows, cols) for _ in range(ITERS - 1)],
                [[vm(rows + 8, cols) for _ in range(frames + 1)] for _ in range(ITERS)],
                [vm(frames + 1, rows, cols) for _ in range(ITERS - 1)],
                [[vm(*block) for _ in range(3)] for _ in range(ITERS - 1)],
                vm(*block),
                vm(3, 8, cols), vm(3, 8, 128), vm(rows, 128), vm(rows, 128),
                vm(ITERS, 8, cols), vm(ITERS, 8, 128),
                vm(ITERS, len(ROW_TO), 8, cols), vm(ITERS, len(COL_TO), 8, 128),
                vm(1, 1, 128), vm(n - 1, 1, 128),
                dma((2,)), dma((ITERS,)), dma((ITERS, groups)),
                dma((1,)), dma((ITERS,)), dma((1,)), dma((ITERS,)),
                dma(()), dma(()),
                pltpu.SemaphoreType.REGULAR((max(1, sum(sizes) - 4),)),
            ],
            compiler_params=pltpu.CompilerParams(
                collective_id=0, has_side_effects=True
            ),
            name="chambolle_pock",
        )(noisy_video, fidelity)
        return pl.pallas_call(
            put,
            out_shape=(
                jax.ShapeDtypeStruct(block, jnp.float32),
                jax.ShapeDtypeStruct((ITERS,), jnp.float32),
            ),
            in_specs=[pl.BlockSpec(memory_space=pltpu.VMEM)] * 2,
            out_specs=[pl.BlockSpec(memory_space=pltpu.HBM)] * 2,
            scratch_shapes=[dma((2,))],
            name="put",
        )(*[pltpu.with_memory_space_constraint(x, pltpu.VMEM) for x in outs])

    return jax.shard_map(
        on_device,
        mesh=mesh,
        in_specs=(P("tm", "row", "col"), P("tm", "row", "col")),
        out_specs=(P("tm", "row", "col"), P()),
        check_vma=False,
    )
```

```python
import functools

import jax
import jax.numpy as jnp
from jax import lax
from jax.experimental import pallas as pl
from jax.experimental.pallas import tpu as pltpu
from jax.sharding import PartitionSpec as P

ITERS = 3
SIGMA = 0.28
TAU = 0.28
MESH = pl.DeviceIdType.MESH

ROW_TO = ((0, -1, 0), (0, 1, 0), (1, -1, 0), (-1, 1, 0))
COL_TO = ((0, 0, -1), (0, 0, 1), (1, 0, -1), (-1, 0, 1), (0, 1, -1), (0, -1, 1))
FRAME_TO = ((-1, 0, 0), (1, 0, 0))


def kernel(
    sizes, groups, early, relays, f_hbm, lam_hbm, out_hbm, gaps_ref,
    ub, lam, inv_lam, inv_den, uus, p0s, p1s, p2s, gus, es,
    pr, pc, hc, mp, sr, sc, rsr, rsc, gsend, grecv,
    ld_sem, fs_sem, fr_sem, rs_sem, rr_sem, cs_sem, cr_sem, gs_sem, gr_sem, hello_sem,
    rbuf, rl_sem, fw_sem,
):
    nt, nr, nc = sizes
    n = nt * nr * nc
    frames, rows, cols = f_hbm.shape
    it, ir, ic = lax.axis_index("tm"), lax.axis_index("row"), lax.axis_index("col")
    me = (it * nr + ir) * nc + ic
    per = rows // groups
    chunks = per // 8
    half = cols // 128
    f32 = jnp.float32

    def exists(off):
        cond = None
        for pos, size, d in zip((it, ir, ic), sizes, off):
            if d:
                c = pos + d < size if d > 0 else pos > 0
                cond = c if cond is None else jnp.logical_and(cond, c)
        return cond

    def place(off):
        return tuple(
            jnp.clip(pos + d, 0, size - 1) if d else pos
            for pos, size, d in zip((it, ir, ic), sizes, off)
        )

    def device(index):
        return (index // (nr * nc), (index // nc) % nr, index % nc)

    def back(off):
        return tuple(-d for d in off)

    def how_many(offsets):
        return sum(jnp.where(exists(off), 1, 0) for off in offsets)

    def wait_for(count, most, sem, region):
        for c in range(1, most + 1):
            @pl.when(count == c)
            def _(c=c):
                pltpu.make_async_copy(region(c), region(c), sem).wait()

    row_out, row_in = how_many(ROW_TO), how_many([back(o) for o in ROW_TO])
    col_out, col_in = how_many(COL_TO), how_many([back(o) for o in COL_TO])
    frame_out = how_many(FRAME_TO)

    barrier = pltpu.get_barrier_semaphore()
    near = ROW_TO + COL_TO + FRAME_TO
    met = how_many(near)
    for src, via, dst, i, slot in relays:
        for a, b in ((src, via), (via, src)):
            met = met + jnp.where(it == a, 1, 0)

            @pl.when(it == a)
            def _(b=b):
                pl.semaphore_signal(
                    barrier, inc=1, device_id=(b, ir, ic), device_id_type=MESH
                )
    for off in near:
        @pl.when(exists(off))
        def _(off=off):
            pl.semaphore_signal(
                barrier, inc=1, device_id=place(off), device_id_type=MESH
            )

    load_f = [
        pltpu.make_async_copy(
            f_hbm.at[t], ub[0].at[t + 1, pl.ds(0, rows), pl.ds(0, cols)], ld_sem.at[0]
        )
        for t in range(frames)
    ]
    load_lam = pltpu.make_async_copy(lam_hbm, lam, ld_sem.at[1])
    for t in range(frames):
        load_f[t].start()
    load_lam.start()

    rounds = [1] * (nr - 2) + [2] * (nc - 1) + [0] * (nt - 1)

    def hello_to(r):
        axis = rounds[r]
        return [tuple(d if a == axis else 0 for a in range(3)) for d in (-1, 1)]

    def say_hello(r):
        if r < len(rounds):
            for off in hello_to(r):
                @pl.when(exists(off))
                def _(off=off):
                    pl.semaphore_signal(
                        hello_sem.at[r], inc=1, device_id=place(off), device_id_type=MESH
                    )

    def hear_hello(r):
        if 0 <= r < len(rounds):
            pl.semaphore_wait(hello_sem.at[r], how_many(hello_to(r)))

    def next_hello(r):
        hear_hello(r - 1)
        say_hello(r)

    def row_copy(k, i):
        return pltpu.make_async_remote_copy(
            sr.at[k], rsr.at[k, i], rs_sem.at[0], rr_sem.at[k],
            device_id=place(ROW_TO[i]), device_id_type=MESH,
        )

    def col_copy(k, i):
        return pltpu.make_async_remote_copy(
            sc.at[k], rsc.at[k, i], cs_sem.at[0], cr_sem.at[k],
            device_id=place(COL_TO[i]), device_id_type=MESH,
        )

    def frame_copy(k, i, g):
        src_frame, dst_frame = ((1, frames + 1), (frames, 0))[i]
        part = pl.ds(pl.multiple_of(g * per, 8), per)
        return pltpu.make_async_remote_copy(
            ub[k].at[src_frame, part, pl.ds(0, cols)],
            ub[k].at[dst_frame, part, pl.ds(0, cols)],
            fs_sem.at[k], fr_sem.at[k, g],
            device_id=place(FRAME_TO[i]), device_id_type=MESH,
        )

    relay_from = groups - groups // 2

    def send_frames(k, g, direct=True):
        for i in (0, 1):
            there = exists(FRAME_TO[i])
            if not direct:
                for src, via, dst, j, slot in relays:
                    if i == j:
                        there = jnp.logical_and(there, it != src)

            @pl.when(there)
            def _(i=i):
                frame_copy(k, i, g).start()

    def send_relay(k, g):
        for src, via, dst, i, slot in relays:
            @pl.when(it == src)
            def _(via=via, i=i, slot=slot):
                part = pl.ds(pl.multiple_of(g * per, 8), per)
                h = g - relay_from
                pltpu.make_async_remote_copy(
                    ub[k].at[(1, frames)[i], part, pl.ds(0, cols)], rbuf.at[slot, k, h],
                    fs_sem.at[k], rl_sem.at[slot, k, h],
                    device_id=(via, ir, ic), device_id_type=MESH,
                ).start()

    def forward(k):
        for src, via, dst, i, slot in relays:
            @pl.when(it == via)
            def _(dst=dst, i=i, slot=slot):
                for g in range(relay_from, groups):
                    box = rbuf.at[slot, k, g - relay_from]
                    pltpu.make_async_copy(box, box, rl_sem.at[slot, k, g - relay_from]).wait()
                    pltpu.make_async_remote_copy(
                        box,
                        ub[k].at[(frames + 1, 0)[i], pl.ds(g * per, per), pl.ds(0, cols)],
                        fw_sem.at[slot], fr_sem.at[k, g],
                        device_id=(dst, ir, ic), device_id_type=MESH,
                    ).start()

    def wait_frames(k, g):
        part = pl.ds(pl.multiple_of(g * per, 8), per)
        wait_for(
            frame_out, 2, fr_sem.at[k, g],
            lambda c: ub[k].at[pl.ds(0, c), part, pl.ds(0, cols)],
        )

    def send_rows(k):
        for t in range(frames):
            sr[k, t : t + 1, :] = ub[k][t + 1, 0:1, 0:cols]
            sr[k, frames + t : frames + t + 1, :] = ub[k][t + 1, rows - 1 : rows, 0:cols]
        for i in range(len(ROW_TO)):
            @pl.when(exists(ROW_TO[i]))
            def _(i=i):
                row_copy(k, i).start()

    def send_cols(k):
        sc[k] = mp[...].T[0:8, :]
        for i in range(len(COL_TO)):
            @pl.when(exists(COL_TO[i]))
            def _(i=i):
                col_copy(k, i).start()

    def send_small(k):
        send_rows(k)
        send_cols(k)

    def wait_small(k):
        wait_for(row_in, len(ROW_TO), rr_sem.at[k], lambda c: rsr.at[k, pl.ds(0, c)])
        wait_for(col_in, len(COL_TO), cr_sem.at[k], lambda c: rsc.at[k, pl.ds(0, c)])

    lane = lax.broadcasted_iota(jnp.int32, (8, 128), 1)
    sub = lax.broadcasted_iota(jnp.int32, (8, 128), 0)
    lane_w = lax.broadcasted_iota(jnp.int32, (8, cols), 1)
    sub_w = lax.broadcasted_iota(jnp.int32, (8, cols), 0)
    end_t, end_r, end_c = it == nt - 1, ir == nr - 1, ic == nc - 1

    def pack_cols(firsts, lasts):
        packed = jnp.zeros((8, 128), f32)
        for t in range(frames):
            packed = jnp.where(lane == t, pltpu.roll(firsts[t], t, 1) if t else firsts[t], packed)
            packed = jnp.where(lane == frames + t, pltpu.roll(lasts[t], frames + t + 1, 1), packed)
        return packed

    loaded = ub[0].at[pl.ds(1, frames), pl.ds(0, rows), pl.ds(0, cols)]
    pltpu.make_async_copy(loaded, loaded, ld_sem.at[0]).wait()

    def first_pack(c, carry):
        r = pl.ds(pl.multiple_of(c * 8, 8), 8)
        mp[r, :] = pack_cols(
            [ub[0][t + 1, r, 0:128] for t in range(frames)],
            [ub[0][t + 1, r, cols - 128 : cols] for t in range(frames)],
        )
        return carry

    lax.fori_loop(0, rows // 8, first_pack, 0, unroll=8)
    pl.semaphore_wait(barrier, met)
    send_small(0)
    if relays:
        for g in range(relay_from, groups):
            send_relay(0, g)
    for g in range(groups):
        send_frames(0, g, g < relay_from)
    say_hello(0)
    load_lam.wait()

    def prepare(c, carry):
        r = pl.ds(pl.multiple_of(c * 8, 8), 8)
        for t in range(frames):
            value = lam[t, r, :]
            inv_lam[t, r, :] = 0.5 / value
            inv_den[t, r, :] = 1.0 / (1.0 + TAU * value)
        return carry

    lax.fori_loop(0, rows // 8, prepare, 0)

    def shrink(m):
        s = jnp.minimum(1.0, lax.rsqrt(m[0] * m[0] + m[1] * m[1] + m[2] * m[2]))
        return [v * s for v in m]

    def edge_duals(k):
        a = rsr[k, 1]
        ahead_t = jnp.where(sub_w == 7, pltpu.roll(rsr[k, 3], 3, 0), pltpu.roll(a, 7, 0))
        corner = pltpu.roll(rsc[k, 4], 4, 0)[:, 127:128]
        ahead_c = jnp.where(lane_w == cols - 1, corner, pltpu.roll(a, cols - 1, 1))
        g = [
            jnp.where(jnp.logical_and(sub_w == 7, end_t), 0.0, ahead_t - a),
            pltpu.roll(sr[k], 4, 0) - a,
            jnp.where(jnp.logical_and(lane_w == cols - 1, end_c), 0.0, ahead_c - a),
        ]
        m = [SIGMA * v if k == 0 else pr[d] + SIGMA * v for d, v in enumerate(g)]
        m = shrink(m)
        for d in range(3):
            pr[d] = m[d]
        above = jnp.where(ir > 0, m[1], 0.0)
        for t in range(frames):
            p1s[k][t + 1][7:8, :] = above[frames + t : frames + t + 1, :]
        b = rsc[k, 1]
        ahead_t = jnp.where(sub == 7, pltpu.roll(rsc[k, 3], 3, 0), pltpu.roll(b, 7, 0))
        corner = rsc[k, 5][:, 0:1]
        ahead_r = jnp.where(lane == 127, corner, pltpu.roll(b, 127, 1))
        g = [
            jnp.where(jnp.logical_and(sub == 7, end_t), 0.0, ahead_t - b),
            jnp.where(jnp.logical_and(lane == 127, end_r), 0.0, ahead_r - b),
            pltpu.roll(sc[k], 4, 0) - b,
        ]
        m = [SIGMA * v if k == 0 else pc[d] + SIGMA * v for d, v in enumerate(g)]
        m = shrink(m)
        for d in range(3):
            pc[d] = m[d]
        left = jnp.where(ic > 0, m[2], 0.0)
        right = jnp.where(sub == frames, pltpu.roll(rsc[k, 2], 1, 0), rsc[k, 0])
        hc[...] = jnp.concatenate(
            [right, left, jnp.zeros((112, 128), f32)], axis=0
        ).T
        for t in range(frames):
            ub[k][t + 1, rows : rows + 1, 0:cols] = rsr[k, 0, t : t + 1, :]
        ub[k][0, rows : rows + 1, 0:cols] = rsr[k, 2, frames - 1 : frames, :]

    def lanes(h):
        return pl.ds(h * 128, 128)

    def gap_term(g, e, noisy, inv, weight, u):
        term = jnp.sqrt(g[0] * g[0] + g[1] * g[1] + g[2] * g[2]) + e * (e * inv + noisy)
        if u is None:
            return term
        resid = u - noisy
        return term + 0.5 * weight * resid * resid

    def chunk(k, c, acc):
        r0 = pl.multiple_of(c * 8, 8)
        r = pl.ds(r0, 8)
        below = pl.ds(pl.multiple_of(r0 + 8, 8), 8)
        last_chunk_row = jnp.logical_and(jnp.logical_and(sub == 7, end_r), c == rows // 8 - 1)
        last_lane = jnp.logical_and(lane == 127, end_c)
        halo = hc[r, :]
        prev0 = None
        firsts, lasts = [], []
        x = [ub[k][0, r, lanes(h)] for h in range(half)]
        for j in range(frames + 1):
            t = j - 1
            xn = [ub[k][j + 1, r, lanes(h)] for h in range(half)]
            where_right = t if t >= 0 else frames
            right = jnp.broadcast_to(halo[:, where_right : where_right + 1], (8, 128))
            cur0, cur2 = [], []
            if t >= 0:
                prev1 = [p1s[k][j][r, lanes(h)] for h in range(half)]
            for h in range(half):
                g0 = xn[h] - x[h]
                if t == frames - 1:
                    g0 = jnp.where(end_t, 0.0, g0)
                g1 = pltpu.roll(jnp.where(sub == 0, ub[k][j, below, lanes(h)], x[h]), 7, 0) - x[h]
                g1 = jnp.where(last_chunk_row, 0.0, g1)
                follow = x[h + 1] if h + 1 < half else right
                g2 = pltpu.roll(jnp.where(lane == 0, follow, x[h]), 127, 1) - x[h]
                if h == half - 1:
                    g2 = jnp.where(last_lane, 0.0, g2)
                g = [g0, g1, g2]
                if k == 0:
                    m = [SIGMA * v for v in g]
                else:
                    m = [
                        p0s[k - 1][j, r, lanes(h)],
                        p1s[k - 1][j][below, lanes(h)],
                        p2s[k - 1][j, r, lanes(h)],
                    ]
                    m = [q + SIGMA * v for q, v in zip(m, g)]
                m = shrink(m)
                if k < ITERS - 1:
                    p0s[k][j, r, lanes(h)] = m[0]
                    p2s[k][j, r, lanes(h)] = m[2]
                p1s[k][j][below, lanes(h)] = m[1]
                cur0.append(m[0])
                cur2.append(m[2])
                if t < 0:
                    continue
                d0 = m[0] - prev0[h]
                d1 = m[1] - pltpu.roll(jnp.where(sub == 7, prev1[h], m[1]), 1, 0)
                if h == 0:
                    before = jnp.broadcast_to(halo[:, 8 + frames + t : 9 + frames + t], (8, 128))
                else:
                    before = cur2[h - 1]
                d2 = m[2] - pltpu.roll(jnp.where(lane == 127, before, m[2]), 1, 1)
                e = d0 + d1 + d2
                if k > 0:
                    g = [0.5 * (v + gus[k - 1][d][t, r, lanes(h)]) for d, v in enumerate(g)]
                if k < ITERS - 1:
                    for d in range(3):
                        gus[k][d][t, r, lanes(h)] = g[d]
                noisy = ub[0][j, r, lanes(h)]
                weight = lam[t, r, lanes(h)]
                u = noisy if k == 0 else uus[k - 1][t, r, lanes(h)]
                if k < ITERS - 1:
                    es[t, r, lanes(h)] = e
                else:
                    acc = acc + gap_term(g, e, noisy, inv_lam[t, r, lanes(h)], weight, u)
                new = (u + TAU * e + TAU * weight * noisy) * inv_den[t, r, lanes(h)]
                (out_hbm if k == ITERS - 1 else uus[k])[t, r, lanes(h)] = new
                if k < ITERS - 1:
                    ubar = 2.0 * new - u
                    ub[k + 1][j, r, lanes(h)] = ubar
                    if h == 0:
                        firsts.append(ubar)
                    if h == half - 1:
                        lasts.append(ubar)
            if t < 0:
                prev0 = [jnp.where(it > 0, v, 0.0) for v in cur0]
            else:
                prev0 = cur0
            x = xn
        if k < ITERS - 1:
            mp[r, :] = pack_cols(firsts, lasts)
        return acc

    def gap_chunk(k, c, acc):
        r = pl.ds(pl.multiple_of(c * 8, 8), 8)
        for t in range(frames):
            for h in range(half):
                at = (t, r, lanes(h))
                noisy = ub[0][t + 1, r, lanes(h)]
                acc = acc + gap_term(
                    [gus[k][d][at] for d in range(3)], es[at], noisy, inv_lam[at],
                    lam[at] if k else None, uus[k - 1][at] if k else None,
                )
        return acc

    local = jnp.zeros((1, 128), f32)
    lane_row = lax.broadcasted_iota(jnp.int32, (1, 128), 1)
    for k in range(ITERS):
        forward(k)
        wait_small(k)
        edge_duals(k)
        next_hello(2 * k + 1)
        wait_frames(k, 0)

        def group(g, acc, k=k):
            @pl.when(g + 1 < groups)
            def _():
                wait_frames(k, g + 1)

            acc = lax.fori_loop(
                0, chunks, lambda c, a: chunk(k, g * chunks + c, a), acc, unroll=2
            )
            if k < ITERS - 1:
                @pl.when(g < early)
                def _():
                    send_frames(k + 1, g)

                if relays:
                    @pl.when(g >= relay_from)
                    def _():
                        send_relay(k + 1, g)
            return acc

        acc = lax.fori_loop(0, groups, group, jnp.zeros((8, 128), f32))
        next_hello(2 * k + 2)
        if k < ITERS - 1:
            send_small(k + 1)
            for g in range(early, groups):
                send_frames(k + 1, g, g < relay_from)
            acc = lax.fori_loop(
                0, rows // 8, functools.partial(gap_chunk, k), acc, unroll=2
            )
        total = jnp.sum(jnp.sum(acc, axis=0, keepdims=True), axis=1, keepdims=True)
        local = jnp.where(lane_row == k, total, local)

    for r in range(2 * ITERS, len(rounds)):
        next_hello(r + 1)

    gsend[0] = local

    def gap_copy(j):
        return pltpu.make_async_remote_copy(
            gsend.at[0], grecv.at[j - 1], gs_sem, gr_sem,
            device_id=device((me + j) % n), device_id_type=MESH,
        )

    def tell(b, carry):
        for c in range(spread):
            gap_copy(b * spread + c + 1).start()
        return carry

    spread = max(d for d in range(1, 33) if (n - 1) % d == 0)
    lax.fori_loop(0, (n - 1) // spread, tell, 0)

    wait_for(row_out, len(ROW_TO), rs_sem.at[0], lambda c: rsr.at[:, pl.ds(0, c)])
    wait_for(col_out, len(COL_TO), cs_sem.at[0], lambda c: rsc.at[:, pl.ds(0, c)])
    for k in range(ITERS):
        wait_for(
            frame_out, 2, fs_sem.at[k],
            lambda c, k=k: ub[k].at[pl.ds(0, c), pl.ds(0, rows), pl.ds(0, cols)],
        )
    for src, via, dst, i, slot in relays:
        @pl.when(it == via)
        def _(slot=slot):
            sent = rbuf.at[slot]
            pltpu.make_async_copy(sent, sent, fw_sem.at[slot]).wait()
    everything = grecv.at[pl.ds(0, n - 1)]
    pltpu.make_async_copy(everything, everything, gr_sem).wait()
    pltpu.make_async_copy(everything, everything, gs_sem).wait()

    total = local + jnp.sum(grecv[...], axis=0)
    total = total * (1.0 / float(n * frames * rows * cols))
    gaps_ref[...] = total[0, 0:ITERS]


def put(u, gaps, u_out, gaps_out, sem):
    copies = [
        pltpu.make_async_copy(u, u_out, sem.at[0]),
        pltpu.make_async_copy(gaps, gaps_out, sem.at[1]),
    ]
    for c in copies:
        c.start()
    for c in copies:
        c.wait()


def corner_relays(mesh):
    at = [getattr(d, "coords", None) for d in mesh.devices[:, 0, 0]]
    relays, busy = [], {}
    if any(c is None for c in at):
        return relays
    at = [tuple(c) for c in at]
    for a in range(len(at) - 1):
        for src, dst, i in ((a, a + 1, 1), (a + 1, a, 0)):
            step = [abs(p - q) for p, q in zip(at[src], at[dst])]
            corner = (at[src][0], at[dst][1], *at[src][2:])
            if step == [1, 1, 0] and corner in at:
                via = at.index(corner)
                slot = busy[via] = busy.get(via, -1) + 1
                relays.append((src, via, dst, i, slot))
    return relays


def solution(mesh):
    sizes = (mesh.shape["tm"], mesh.shape["row"], mesh.shape["col"])
    n = sizes[0] * sizes[1] * sizes[2]
    relays = corner_relays(mesh)
    slots = 1 + max([slot for *_, slot in relays], default=0)

    def on_device(noisy_video, fidelity):
        frames, rows, cols = noisy_video.shape
        groups = 8
        early = 4
        held = groups // 2
        block = (frames, rows, cols)
        dma = pltpu.SemaphoreType.DMA
        vm = lambda *shape: pltpu.VMEM(shape, jnp.float32)
        outs = pl.pallas_call(
            functools.partial(kernel, sizes, groups, early, relays),
            out_shape=(
                pltpu.VMEM(block, jnp.float32),
                pltpu.VMEM((ITERS,), jnp.float32),
            ),
            in_specs=[pl.BlockSpec(memory_space=pltpu.HBM)] * 2,
            out_specs=(
                pl.BlockSpec(memory_space=pltpu.VMEM),
                pl.BlockSpec(memory_space=pltpu.VMEM),
            ),
            scratch_shapes=[
                [vm(frames + 2, rows + 8, cols) for _ in range(ITERS)],
                vm(*block), vm(*block), vm(*block),
                [vm(*block) for _ in range(ITERS)],
                [vm(frames + 1, rows, cols) for _ in range(ITERS - 1)],
                [[vm(rows + 8, cols) for _ in range(frames + 1)] for _ in range(ITERS)],
                [vm(frames + 1, rows, cols) for _ in range(ITERS - 1)],
                [[vm(*block) for _ in range(3)] for _ in range(ITERS - 1)],
                vm(*block),
                vm(3, 8, cols), vm(3, 8, 128), vm(rows, 128), vm(rows, 128),
                vm(ITERS, 8, cols), vm(ITERS, 8, 128),
                vm(ITERS, len(ROW_TO), 8, cols), vm(ITERS, len(COL_TO), 8, 128),
                vm(1, 1, 128), vm(n - 1, 1, 128),
                dma((2,)), dma((ITERS,)), dma((ITERS, groups)),
                dma((1,)), dma((ITERS,)), dma((1,)), dma((ITERS,)),
                dma(()), dma(()),
                pltpu.SemaphoreType.REGULAR((max(1, sum(sizes) - 4),)),
                vm(slots, ITERS, held, rows // groups, cols),
                dma((slots, ITERS, held)), dma((slots,)),
            ],
            compiler_params=pltpu.CompilerParams(
                collective_id=0, has_side_effects=True
            ),
            name="chambolle_pock",
        )(noisy_video, fidelity)
        return pl.pallas_call(
            put,
            out_shape=(
                jax.ShapeDtypeStruct(block, jnp.float32),
                jax.ShapeDtypeStruct((ITERS,), jnp.float32),
            ),
            in_specs=[pl.BlockSpec(memory_space=pltpu.VMEM)] * 2,
            out_specs=[pl.BlockSpec(memory_space=pltpu.HBM)] * 2,
            scratch_shapes=[dma((2,))],
            name="put",
        )(*[pltpu.with_memory_space_constraint(x, pltpu.VMEM) for x in outs])

    return jax.shard_map(
        on_device,
        mesh=mesh,
        in_specs=(P("tm", "row", "col"), P("tm", "row", "col")),
        out_specs=(P("tm", "row", "col"), P()),
        check_vma=False,
    )
```
